32 devices in a mesh: ta: 4 (over y, x), gy: 2 (over core), gx: 4 (over z).
Axes of the slice: x: 2, y: 2, z: 4, core: 2. Of those that a mesh axis runs over, the one named last changes fastest.
Arguments:
- features: bfloat16 [16, 4, 416, 192], P('ta', 'gy', 'gx'), may hold values from -6 to 6
- gain_first: float32 [192], replicated, may hold values from 0.1 to 1.9
- kernel_first: bfloat16 [3, 3, 3, 192, 192], replicated, may hold values from -0.078125 to 0.078125
- bias_first: float32 [192], replicated, may hold values from -3 to 3
- gain_second: float32 [192], replicated, may hold values from 0.1 to 1.9
- kernel_second: bfloat16 [3, 3, 3, 192, 192], replicated, may hold values from -0.078125 to 0.078125
- bias_second: float32 [192], replicated, may hold values from -3 to 3
Outputs:
- block_out: bfloat16 [16, 4, 416, 192], P('ta', 'gy', 'gx')
The draws below stay inside these ranges and needn't reach their ends.
All inputs are finite; a program needn't handle non-finite values.
Results may differ from the reference program's by a relative error of at most 0.0075.
Values may be sent and summed in bfloat16 or wider, within the bound.
A program may use at most 64 MiB of HBM per device.

```python
import jax
import jax.numpy as jnp
from jax import lax

C = 192
W = 416
FRAMES = 16
H = 4


def levels(stream_key, dims, split, low, top_value):
    level = 1.0
    for dim, parts in split:
        heights = jax.random.uniform(jax.random.fold_in(jax.random.fold_in(stream_key, 6), dim), (parts,), jnp.float32, low / len(split), top_value / len(split))
        level = level * jnp.repeat(jnp.exp(heights), dims[dim] // parts).reshape((-1,) + (1,) * (len(dims) - 1 - dim))
    return level


def bell_draw(stream_key, dims, spread, bound, cuts=(), kind=jnp.bfloat16):
    factor_of = levels(stream_key, dims, cuts, -0.22, 0.18) if cuts else 1.0
    array = jax.random.normal(stream_key, dims, jnp.float32) * spread * factor_of
    return jnp.minimum(jnp.maximum(array, -bound), bound).astype(kind)


def setup_inputs(seed: int = 0) -> dict:
    streams_of = jax.random.split(jax.random.key(seed), 8)
    features = bell_draw(streams_of[0], (FRAMES, H, W, C), 1.0, 6.0, ((0, 4), (1, 2), (2, 4)))
    gain_first = jnp.clip(1.0 + 0.18 * jax.random.normal(streams_of[1], (C,), jnp.float32), 0.1, 1.9)
    kernel_first = bell_draw(streams_of[2], (3, 3, 3, C, C), (27 * C) ** -0.5, 0.078125)
    bias_first = bell_draw(streams_of[3], (C,), 0.5, 3.0, (), jnp.float32)
    gain_second = jnp.clip(1.0 + 0.18 * jax.random.normal(streams_of[4], (C,), jnp.float32), 0.1, 1.9)
    kernel_second = bell_draw(streams_of[5], (3, 3, 3, C, C), (27 * C) ** -0.5, 0.078125)
    bias_second = bell_draw(streams_of[6], (C,), 0.5, 3.0, (), jnp.float32)
    return dict(features=features, gain_first=gain_first, kernel_first=kernel_first, bias_first=bias_first, gain_second=gain_second, kernel_second=kernel_second, bias_second=bias_second)


epsilon = 1e-06

def activate(field, gain):
    field = field.astype(jnp.float32)
    meansq = lax.optimization_barrier(jnp.mean(field * field, axis=-1, keepdims=True))
    return jax.nn.silu(field * lax.rsqrt(meansq + epsilon) * gain).astype(jnp.bfloat16)

def convolve(source, kernel, bias):
    frames, rows, cols, channels = source.shape
    padded = jnp.pad(source, ((2, 0), (1, 1), (1, 1), (0, 0)))

    def one_frame(index):
        window = lax.dynamic_slice_in_dim(padded, index, 3, 0)
        total = jnp.zeros((rows * cols, kernel.shape[-1]), jnp.float32)
        for delta_t in range(3):
            for delta_y in range(3):
                for delta_x in range(3):
                    piece = window[delta_t, delta_y:delta_y + rows, delta_x:delta_x + cols].reshape(-1, channels)
                    total = total + jnp.dot(piece, kernel[delta_t, delta_y, delta_x], preferred_element_type=jnp.float32)
        return total.reshape(rows, cols, -1) + bias
    return lax.map(one_frame, jnp.arange(frames, dtype=jnp.int32))

def reference(features, gain_first, kernel_first, bias_first, gain_second, kernel_second, bias_second):
    first = activate(features, gain_first)
    middle = convolve(first, kernel_first, bias_first).astype(jnp.bfloat16)
    second = activate(middle, gain_second)
    result = convolve(second, kernel_second, bias_second) + features.astype(jnp.float32)
    return result.astype(jnp.bfloat16)
```

```python
import functools

import jax
import jax.numpy as jnp
from jax import lax
from jax.experimental import pallas as pl
from jax.experimental.pallas import tpu as pltpu
from jax.sharding import PartitionSpec as P

epsilon = 1e-06
LATE, EARLY, PAST = 0, 1, 2
MOVES = [(dy, dx) for dy in (-1, 0, 1) for dx in (-1, 0, 1)]


def moves_of(kind):
    return [m for m in MOVES if kind == PAST or m != (0, 0)]


def activate(field, gain):
    meansq = jnp.mean(field * field, axis=-1, keepdims=True)
    u = field * lax.rsqrt(meansq + epsilon) * gain
    return u / (1.0 + jnp.exp(-u))


def block_kernel(
    feat, gain1, bias1, gain2, bias2, k1, k2, out,
    weights, act, edges, main_in, row_in, edge_in, line, cols3, acc,
    w_sem, send_sem, recv_sem,
):
    rows, cols, ch = feat.shape[1:]
    colsp = acc.shape[0] // (2 * rows)
    lanes = line.shape[-1]
    ta, gy, gx = (lax.axis_index(a) for a in ("ta", "gy", "gx"))
    n_ta, n_gy, n_gx = (lax.axis_size(a) for a in ("ta", "gy", "gx"))

    def inside(kind, dy, dx, sign):
        t = ta + sign * (1 if kind == PAST else 0)
        y, x = gy + sign * dy, gx + sign * dx
        ok = (t >= 0) & (t < n_ta) & (y >= 0) & (y < n_gy) & (x >= 0) & (x < n_gx)
        return ok, {"ta": t, "gy": y, "gx": x}

    w_copies = [
        pltpu.make_async_copy(k, weights.at[layer, :, pl.ds(0, ch)], w_sem.at[layer])
        for layer, k in enumerate((k1, k2))
    ]
    w_copies[0].start()
    w_copies[1].start()

    barrier = pltpu.get_barrier_semaphore()
    expected = jnp.int32(0)
    for kind in (LATE, PAST):
        for dy, dx in moves_of(kind):
            ok, source = inside(kind, dy, dx, -1)

            @pl.when(ok)
            def _():
                pl.semaphore_signal(
                    barrier, inc=1, device_id=source, device_id_type=pl.DeviceIdType.MESH
                )

            expected = expected + inside(kind, dy, dx, 1)[0].astype(jnp.int32)

    def landing(layer, kind, dy, dx):
        if dx:
            return edge_in.at[layer, kind, dy + 1, (dx + 1) // 2]
        if dy:
            return row_in.at[layer, kind, (dy + 1) // 2]
        return main_in.at[layer]

    def copy_of(layer, kind, dy, dx):
        half = EARLY if kind == EARLY else LATE
        frame = 0 if kind == EARLY else 2
        if dx:
            src = edges.at[layer, half, (dx + 1) // 2]
        elif dy:
            src = act.at[layer, pl.ds(frame, 2), rows - 1 if dy > 0 else 0]
        else:
            src = act.at[layer, pl.ds(frame, 2)]
        number = kind * 9 + (dy + 1) * 3 + dx + 1
        ok, target = inside(kind, dy, dx, 1)
        return ok, pltpu.make_async_remote_copy(
            src_ref=src,
            dst_ref=landing(layer, kind, dy, dx),
            send_sem=send_sem.at[layer, number],
            recv_sem=recv_sem.at[layer, number],
            device_id=target,
            device_id_type=pl.DeviceIdType.MESH,
        )

    def send(layer, kind):
        for dy, dx in sorted(moves_of(kind), key=lambda m: (m[1] != 0, m)):
            ok, copy = copy_of(layer, kind, dy, dx)
            pl.when(ok)(copy.start)

    def receive(layer, kind):
        for dy, dx in moves_of(kind):
            ok, _ = inside(kind, dy, dx, -1)
            copy = copy_of(layer, kind, dy, dx)[1]
            place = landing(layer, kind, dy, dx)
            pl.when(ok)(copy.wait_recv)

            @pl.when(jnp.logical_not(ok))
            def _():
                place[...] = jnp.zeros_like(place)

    def keep(layer, frame, row, value):
        half = LATE if frame >= 2 else EARLY
        act[layer, frame, row] = value.astype(jnp.bfloat16)
        value = value.astype(jnp.bfloat16).astype(jnp.float32)
        at = (frame % 2) * rows + row
        edges[layer, half, 0, at : at + 1, :] = value[0:1]
        edges[layer, half, 1, at : at + 1, :] = value[cols - 1 : cols]

    def spread(layer, kind):
        base = {LATE: 4, EARLY: 2, PAST: 0}[kind]
        for f in range(2):
            for row in range(-1, rows + 1):
                if row < 0 or row >= rows:
                    dy = 1 if row < 0 else -1
                    source = row_in[layer, kind, (dy + 1) // 2, f]
                    at = f * rows + (rows - 1 if row < 0 else 0)
                else:
                    dy = 0
                    at = f * rows + row
                    if kind == PAST:
                        source = main_in[layer, f, row]
                    else:
                        source = act[layer, base - 2 + f, row]
                slot = f * (rows + 2) + row + 1
                line[slot, 8 : 8 + cols, 0:ch] = source.astype(jnp.float32)
                line[slot, 7:8, 0:ch] = edge_in[layer, kind, dy + 1, 1, at : at + 1, :]
                line[slot, 8 + cols : 9 + cols, 0:ch] = edge_in[layer, kind, dy + 1, 0, at : at + 1, :]
                for r in range(3):
                    cols3[layer, base + f, row + 1, 0:cols, r * lanes : (r + 1) * lanes] = line[
                        slot, 7 + r : 7 + r + cols, :
                    ].astype(jnp.bfloat16)

    def convolve(layer, frame):
        def tap(p, _):
            total = None
            for q in range(3):
                piece = cols3[layer, pl.ds(frame + p, 2), q : q + rows].reshape(-1, 3 * lanes)
                kernel = weights[layer, pl.ds(9 * p + 3 * q, 3)].reshape(3 * lanes, ch)
                part = jnp.dot(piece, kernel, preferred_element_type=jnp.float32)
                total = part if total is None else total + part
            acc[...] += total
            return 0

        acc[...] = jnp.zeros_like(acc)
        lax.fori_loop(0, 3, tap, 0)

    def cells(f, row):
        at = (f * rows + row) * colsp
        return acc[at : at + cols, :]

    def middle(frame):
        for f in range(2):
            for row in range(rows):
                value = (cells(f, row) + bias1[...]).astype(jnp.bfloat16).astype(jnp.float32)
                keep(1, frame + f, row, activate(value, gain2[...]))

    def finish(frame):
        for f in range(2):
            for row in range(rows):
                value = cells(f, row) + bias2[...] + feat[frame + f, row].astype(jnp.float32)
                out[frame + f, row] = value.astype(jnp.bfloat16)

    def first(frame):
        for f in range(2):
            for row in range(rows):
                keep(0, frame + f, row, activate(feat[frame + f, row].astype(jnp.float32), gain1[...]))

    edges[...] = jnp.zeros_like(edges)
    first(2)
    pl.semaphore_wait(barrier, expected)
    send(0, PAST)
    send(0, LATE)
    first(0)
    send(0, EARLY)
    weights[:, :, ch:, :] = jnp.zeros((2, weights.shape[1], lanes - ch, ch), jnp.bfloat16)
    line[...] = jnp.zeros_like(line)
    receive(0, LATE)
    spread(0, LATE)
    receive(0, EARLY)
    spread(0, EARLY)
    w_copies[0].wait()
    convolve(0, 2)
    middle(2)
    send(1, PAST)
    send(1, LATE)
    receive(0, PAST)
    spread(0, PAST)
    convolve(0, 0)
    middle(0)
    send(1, EARLY)
    receive(1, LATE)
    spread(1, LATE)
    receive(1, EARLY)
    spread(1, EARLY)
    w_copies[1].wait()
    convolve(1, 2)
    finish(2)
    receive(1, PAST)
    spread(1, PAST)
    convolve(1, 0)
    finish(0)
    for layer in range(2):
        for kind in (LATE, EARLY, PAST):
            for dy, dx in moves_of(kind):
                ok, copy = copy_of(layer, kind, dy, dx)
                pl.when(ok)(copy.wait_send)


def local(features, gain_first, kernel_first, bias_first, gain_second, kernel_second, bias_second):
    frames, rows, cols, ch = features.shape
    colsp = -(-cols // 16) * 16
    lanes = -(-ch // 128) * 128
    vmem = pl.BlockSpec(memory_space=pltpu.VMEM)
    hbm = pl.BlockSpec(memory_space=pl.ANY)
    edge_rows = -(-2 * rows // 8) * 8
    bf16, f32 = jnp.bfloat16, jnp.float32
    return pl.pallas_call(
        block_kernel,
        out_shape=jax.ShapeDtypeStruct(features.shape, bf16),
        in_specs=[vmem] * 5 + [hbm] * 2,
        out_specs=vmem,
        scratch_shapes=[
            pltpu.VMEM((2, 27, lanes, ch), bf16),
            pltpu.VMEM((2, frames, rows, cols, ch), bf16),
            pltpu.VMEM((2, 2, 2, edge_rows, ch), f32),
            pltpu.VMEM((2, 2, rows, cols, ch), bf16),
            pltpu.VMEM((2, 3, 2, 2, cols, ch), bf16),
            pltpu.VMEM((2, 3, 3, 2, edge_rows, ch), f32),
            pltpu.VMEM((2 * (rows + 2), cols + 16, lanes), f32),
            pltpu.VMEM((2, frames + 2, rows + 2, colsp, 3 * lanes), bf16),
            pltpu.VMEM((2 * rows * colsp, ch), f32),
            pltpu.SemaphoreType.DMA((2,)),
            pltpu.SemaphoreType.DMA((2, 27)),
            pltpu.SemaphoreType.DMA((2, 27)),
        ],
        compiler_params=pltpu.CompilerParams(
            collective_id=0, has_side_effects=True, vmem_limit_bytes=56 * 1024 * 1024
        ),
        name="residual_block",
    )(
        features,
        gain_first.reshape(1, ch),
        bias_first.reshape(1, ch),
        gain_second.reshape(1, ch),
        bias_second.reshape(1, ch),
        kernel_first.reshape(27, ch, ch),
        kernel_second.reshape(27, ch, ch),
    )


def solution(mesh):
    placed = (P("ta", "gy", "gx", None), P(), P(), P(), P(), P(), P())
    return jax.shard_map(
        local, mesh=mesh, in_specs=placed, out_specs=P("ta", "gy", "gx", None), check_vma=False
    )
```

```python
import functools

import jax
import jax.numpy as jnp
from jax import lax
from jax.experimental import pallas as pl
from jax.experimental.pallas import tpu as pltpu
from jax.sharding import PartitionSpec as P

epsilon = 1e-06
LATE, EARLY, PAST = 0, 1, 2
TILE = 128
MOVES = [(dy, dx) for dy in (-1, 0, 1) for dx in (-1, 0, 1)]


def moves_of(kind):
    return [m for m in MOVES if kind == PAST or m != (0, 0)]


def activate(field, gain):
    meansq = jnp.mean(field * field, axis=-1, keepdims=True)
    u = field * lax.rsqrt(meansq + epsilon) * gain
    return u / (1.0 + jnp.exp(-u))


def block_kernel(
    feat, gain1, bias1, gain2, bias2, k1, k2, out,
    weights, act, edges, main_in, row_in, edge_in, line, cols3, acc,
    w_sem, send_sem, recv_sem,
):
    rows, cols, ch = feat.shape[1:]
    colsp = acc.shape[1] // (2 * rows)
    lanes = line.shape[-1]
    ta, gy, gx = (lax.axis_index(a) for a in ("ta", "gy", "gx"))
    n_ta, n_gy, n_gx = (lax.axis_size(a) for a in ("ta", "gy", "gx"))

    def inside(kind, dy, dx, sign):
        relayed = kind == PAST and dy != 0 and dx == 0
        t = ta + sign * (1 if kind == PAST and not relayed else 0)
        y, x = gy + sign * dy, gx + sign * dx
        ok = (t >= 0) & (t < n_ta) & (y >= 0) & (y < n_gy) & (x >= 0) & (x < n_gx)
        if relayed:
            ok = ok & (ta > 0)
        return ok, {"ta": t, "gy": y, "gx": x}

    w_copies = [
        pltpu.make_async_copy(k, weights.at[layer, :, pl.ds(0, ch)], w_sem.at[layer])
        for layer, k in enumerate((k1, k2))
    ]
    w_copies[0].start()
    w_copies[1].start()

    barrier = pltpu.get_barrier_semaphore()
    expected = jnp.int32(0)
    for kind in (LATE, PAST):
        for dy, dx in moves_of(kind):
            if kind == PAST and dx == 0 and dy != 0:
                continue
            ok, source = inside(kind, dy, dx, -1)

            @pl.when(ok)
            def _():
                pl.semaphore_signal(
                    barrier, inc=1, device_id=source, device_id_type=pl.DeviceIdType.MESH
                )

            expected = expected + inside(kind, dy, dx, 1)[0].astype(jnp.int32)

    def landing(layer, kind, dy, dx):
        if dx:
            return edge_in.at[layer, kind, dy + 1, (dx + 1) // 2]
        if dy:
            return row_in.at[layer, kind, (dy + 1) // 2]
        return main_in.at[layer]

    def copy_of(layer, kind, dy, dx):
        half = EARLY if kind == EARLY else LATE
        if dx:
            src = edges.at[layer, half, (dx + 1) // 2]
        elif dy:
            edge_row = rows - 1 if dy > 0 else 0
            if kind == PAST:
                src = main_in.at[layer, :, edge_row]
            else:
                src = act.at[layer, half, :, edge_row]
        else:
            src = act.at[layer, LATE]
        number = kind * 9 + (dy + 1) * 3 + dx + 1
        ok, target = inside(kind, dy, dx, 1)
        return ok, pltpu.make_async_remote_copy(
            src_ref=src,
            dst_ref=landing(layer, kind, dy, dx),
            send_sem=send_sem.at[layer, number],
            recv_sem=recv_sem.at[layer, number],
            device_id=target,
            device_id_type=pl.DeviceIdType.MESH,
        )

    def send(layer, moves):
        for kind, dy, dx in moves:
            ok, copy = copy_of(layer, kind, dy, dx)
            pl.when(ok)(copy.start)

    def send_late(layer):
        send(layer, [(LATE, -1, 0), (LATE, 1, 0)])
        send(layer, [(kind, *m) for kind in (LATE, PAST) for m in MOVES if m[1]])
        send(layer, [(PAST, 0, 0)])

    def send_early(layer):
        send(layer, [(EARLY, *m) for m in sorted(moves_of(EARLY), key=lambda m: (m[1] != 0, m))])

    def receive(layer, kind, moves):
        for dy, dx in moves:
            ok, _ = inside(kind, dy, dx, -1)
            copy = copy_of(layer, kind, dy, dx)[1]
            place = landing(layer, kind, dy, dx)
            pl.when(ok)(copy.wait_recv)

            @pl.when(jnp.logical_not(ok))
            def _():
                place[...] = jnp.zeros_like(place)

    def receive_past(layer):
        receive(layer, PAST, [(0, 0)])
        send(layer, [(PAST, -1, 0), (PAST, 1, 0)])
        receive(layer, PAST, [m for m in moves_of(PAST) if m != (0, 0)])

    def keep(layer, half, row, values):
        for f, value in enumerate(values):
            packed = value.astype(jnp.bfloat16)
            act[layer, half, f, row] = packed[:, 0:TILE]
            value = packed.astype(jnp.float32)
            at = f * rows + row
            edges[layer, half, 0, at : at + 1, :] = value[0:1]
            edges[layer, half, 1, at : at + 1, :] = value[cols - 1 : cols]
        tails = jnp.concatenate([value[:, TILE:ch] for value in values], axis=1)
        act[layer, half, 2, row] = tails.astype(jnp.bfloat16)

    def spread(layer, kind):
        base = {LATE: 4, EARLY: 2, PAST: 0}[kind]
        for row in range(-1, rows + 1):
            if row < 0 or row >= rows:
                dy = 1 if row < 0 else -1
                source = row_in.at[layer, kind, (dy + 1) // 2]
                edge_row = rows - 1 if row < 0 else 0
            else:
                dy = 0
                source = main_in.at[layer, :, row] if kind == PAST else act.at[layer, kind, :, row]
                edge_row = row
            tails = source[2].astype(jnp.float32)
            for f in range(2):
                at = f * rows + edge_row
                slot = f * (rows + 2) + row + 1
                line[slot, 8 : 8 + cols, 0:TILE] = source[f].astype(jnp.float32)
                line[slot, 8 : 8 + cols, TILE:lanes] = pltpu.roll(tails, TILE // 2, 1) if f else tails
                line[slot, 7:8, 0:ch] = edge_in[layer, kind, dy + 1, 1, at : at + 1, :]
                line[slot, 8 + cols : 9 + cols, 0:ch] = edge_in[layer, kind, dy + 1, 0, at : at + 1, :]
                for r in range(3):
                    cols3[layer, base + f, row + 1, 0:cols, r * lanes : (r + 1) * lanes] = line[
                        slot, 7 + r : 7 + r + cols, :
                    ].astype(jnp.bfloat16)

    def convolve(layer, frame, own):
        total_at = acc.at[1 if frame else 0]

        def product(p):
            total = None
            for q in range(3):
                piece = cols3[layer, pl.ds(frame + p, 2), q : q + rows].reshape(-1, 3 * lanes)
                kernel = weights[layer, pl.ds(9 * p + 3 * q, 3)].reshape(3 * lanes, ch)
                part = jnp.dot(piece, kernel, preferred_element_type=jnp.float32)
                total = part if total is None else total + part
            return total

        def tap(p, _):
            total_at[...] += product(p)
            return 0

        if own:
            total_at[...] = product(2)
        else:
            lax.fori_loop(0, 2, tap, 0)

    def cells(half, f, row):
        at = (f * rows + row) * colsp
        return acc[1 - half, at : at + cols, :]

    def middle(half):
        for row in range(rows):
            values = []
            for f in range(2):
                value = (cells(half, f, row) + bias1[...]).astype(jnp.bfloat16).astype(jnp.float32)
                values.append(activate(value, gain2[...]))
            keep(1, half, row, values)

    def finish(half):
        frame = 0 if half == EARLY else 2
        for f in range(2):
            for row in range(rows):
                value = cells(half, f, row) + bias2[...] + feat[frame + f, row].astype(jnp.float32)
                out[frame + f, row] = value.astype(jnp.bfloat16)

    def first(half):
        frame = 0 if half == EARLY else 2
        for row in range(rows):
            keep(0, half, row, [
                activate(feat[frame + f, row].astype(jnp.float32), gain1[...]) for f in range(2)
            ])

    edges[...] = jnp.zeros_like(edges)
    first(LATE)
    pl.semaphore_wait(barrier, expected)
    send_late(0)
    first(EARLY)
    send_early(0)
    weights[:, :, ch:, :] = jnp.zeros((2, weights.shape[1], lanes - ch, ch), jnp.bfloat16)
    line[...] = jnp.zeros_like(line)
    receive(0, LATE, moves_of(LATE))
    spread(0, LATE)
    w_copies[0].wait()
    convolve(0, 2, True)
    receive(0, EARLY, moves_of(EARLY))
    spread(0, EARLY)
    convolve(0, 2, False)
    middle(LATE)
    send_late(1)
    convolve(0, 0, True)
    w_copies[1].wait()
    receive(1, LATE, moves_of(LATE))
    spread(1, LATE)
    convolve(1, 2, True)
    receive_past(0)
    spread(0, PAST)
    convolve(0, 0, False)
    middle(EARLY)
    send_early(1)
    receive(1, EARLY, moves_of(EARLY))
    spread(1, EARLY)
    convolve(1, 2, False)
    finish(LATE)
    convolve(1, 0, True)
    receive_past(1)
    spread(1, PAST)
    convolve(1, 0, False)
    finish(EARLY)
    for layer in range(2):
        for kind in (LATE, EARLY, PAST):
            for dy, dx in moves_of(kind):
                ok, copy = copy_of(layer, kind, dy, dx)
                pl.when(ok)(copy.wait_send)


def local(features, gain_first, kernel_first, bias_first, gain_second, kernel_second, bias_second):
    frames, rows, cols, ch = features.shape
    colsp = -(-cols // 16) * 16
    lanes = -(-ch // 128) * 128
    vmem = pl.BlockSpec(memory_space=pltpu.VMEM)
    hbm = pl.BlockSpec(memory_space=pl.ANY)
    edge_rows = -(-2 * rows // 8) * 8
    bf16, f32 = jnp.bfloat16, jnp.float32
    return pl.pallas_call(
        block_kernel,
        out_shape=jax.ShapeDtypeStruct(features.shape, bf16),
        in_specs=[vmem] * 5 + [hbm] * 2,
        out_specs=vmem,
        scratch_shapes=[
            pltpu.VMEM((2, 27, lanes, ch), bf16),
            pltpu.VMEM((2, 2, 3, rows, cols, TILE), bf16),
            pltpu.VMEM((2, 2, 2, edge_rows, ch), f32),
            pltpu.VMEM((2, 3, rows, cols, TILE), bf16),
            pltpu.VMEM((2, 3, 2, 3, cols, TILE), bf16),
            pltpu.VMEM((2, 3, 3, 2, edge_rows, ch), f32),
            pltpu.VMEM((2 * (rows + 2), cols + 16, lanes), f32),
            pltpu.VMEM((2, frames + 2, rows + 2, colsp, 3 * lanes), bf16),
            pltpu.VMEM((2, 2 * rows * colsp, ch), f32),
            pltpu.SemaphoreType.DMA((2,)),
            pltpu.SemaphoreType.DMA((2, 27)),
            pltpu.SemaphoreType.DMA((2, 27)),
        ],
        compiler_params=pltpu.CompilerParams(
            collective_id=0, has_side_effects=True, vmem_limit_bytes=56 * 1024 * 1024
        ),
        name="residual_block",
    )(
        features,
        gain_first.reshape(1, ch),
        bias_first.reshape(1, ch),
        gain_second.reshape(1, ch),
        bias_second.reshape(1, ch),
        kernel_first.reshape(27, ch, ch),
        kernel_second.reshape(27, ch, ch),
    )


def solution(mesh):
    placed = (P("ta", "gy", "gx", None), P(), P(), P(), P(), P(), P())
    return jax.shard_map(
        local, mesh=mesh, in_specs=placed, out_specs=P("ta", "gy", "gx", None), check_vma=False
    )
```

```python
import functools

import jax
import jax.numpy as jnp
from jax import lax
from jax.experimental import pallas as pl
from jax.experimental.pallas import tpu as pltpu
from jax.sharding import PartitionSpec as P

epsilon = 1e-06
LATE, EARLY, PAST = 0, 1, 2
TILE = 128
MOVES = [(dy, dx) for dy in (-1, 0, 1) for dx in (-1, 0, 1)]


def moves_of(kind):
    return [m for m in MOVES if kind == PAST or m != (0, 0)]


def activate(field, gain):
    meansq = jnp.mean(field * field, axis=-1, keepdims=True)
    u = field * lax.rsqrt(meansq + epsilon) * gain
    return u / (1.0 + jnp.exp(-u))


def block_kernel(
    feat, gain1, bias1, gain2, bias2, k1, k2, out,
    weights, act, edges, main_in, row_in, edge_in, line, cols3, acc,
    w_sem, send_sem, recv_sem,
):
    rows, ch, cols = feat.shape[1:]
    colsp = acc.shape[1] // (2 * rows)
    lanes = line.shape[-1]
    ta, gy, gx = (lax.axis_index(a) for a in ("ta", "gy", "gx"))
    n_ta, n_gy, n_gx = (lax.axis_size(a) for a in ("ta", "gy", "gx"))

    def inside(kind, dy, dx, sign):
        relayed = kind == PAST and dy != 0 and dx == 0
        t = ta + sign * (1 if kind == PAST and not relayed else 0)
        y, x = gy + sign * dy, gx + sign * dx
        ok = (t >= 0) & (t < n_ta) & (y >= 0) & (y < n_gy) & (x >= 0) & (x < n_gx)
        if relayed:
            ok = ok & (ta > 0)
        return ok, {"ta": t, "gy": y, "gx": x}

    w_copies = [
        pltpu.make_async_copy(k, weights.at[layer, :, pl.ds(0, ch)], w_sem.at[layer])
        for layer, k in enumerate((k1, k2))
    ]
    w_copies[0].start()
    w_copies[1].start()

    barrier = pltpu.get_barrier_semaphore()
    expected = jnp.int32(0)
    for kind in (LATE, PAST):
        for dy, dx in moves_of(kind):
            if kind == PAST and dx == 0 and dy != 0:
                continue
            ok, source = inside(kind, dy, dx, -1)

            @pl.when(ok)
            def _():
                pl.semaphore_signal(
                    barrier, inc=1, device_id=source, device_id_type=pl.DeviceIdType.MESH
                )

            expected = expected + inside(kind, dy, dx, 1)[0].astype(jnp.int32)

    def landing(layer, kind, dy, dx):
        if dx:
            return edge_in.at[layer, kind, dy + 1, (dx + 1) // 2]
        if dy:
            return row_in.at[layer, kind, (dy + 1) // 2]
        return main_in.at[layer]

    def copy_of(layer, kind, dy, dx):
        half = EARLY if kind == EARLY else LATE
        if dx:
            src = edges.at[layer, half, (dx + 1) // 2]
        elif dy:
            edge_row = rows - 1 if dy > 0 else 0
            if kind == PAST:
                src = main_in.at[layer, :, edge_row]
            else:
                src = act.at[layer, half, :, edge_row]
        else:
            src = act.at[layer, LATE]
        number = kind * 9 + (dy + 1) * 3 + dx + 1
        ok, target = inside(kind, dy, dx, 1)
        return ok, pltpu.make_async_remote_copy(
            src_ref=src,
            dst_ref=landing(layer, kind, dy, dx),
            send_sem=send_sem.at[layer, number],
            recv_sem=recv_sem.at[layer, number],
            device_id=target,
            device_id_type=pl.DeviceIdType.MESH,
        )

    def send(layer, moves):
        for kind, dy, dx in moves:
            ok, copy = copy_of(layer, kind, dy, dx)
            pl.when(ok)(copy.start)

    def send_late(layer):
        send(layer, [(LATE, -1, 0), (LATE, 1, 0)])
        send(layer, [(kind, *m) for kind in (LATE, PAST) for m in MOVES if m[1]])
        send(layer, [(PAST, 0, 0)])

    def send_early(layer):
        send(layer, [(EARLY, *m) for m in sorted(moves_of(EARLY), key=lambda m: (m[1] != 0, m))])

    def receive(layer, kind, moves):
        for dy, dx in moves:
            ok, _ = inside(kind, dy, dx, -1)
            copy = copy_of(layer, kind, dy, dx)[1]
            place = landing(layer, kind, dy, dx)
            pl.when(ok)(copy.wait_recv)

            @pl.when(jnp.logical_not(ok))
            def _():
                place[...] = jnp.zeros_like(place)

    def receive_past(layer):
        receive(layer, PAST, [(0, 0)])
        send(layer, [(PAST, -1, 0), (PAST, 1, 0)])
        receive(layer, PAST, [m for m in moves_of(PAST) if m != (0, 0)])

    def keep(layer, half, row, values):
        for f, value in enumerate(values):
            packed = value.astype(jnp.bfloat16)
            act[layer, half, f, row] = packed[:, 0:TILE]
            value = packed.astype(jnp.float32)
            at = f * rows + row
            edges[layer, half, 0, at : at + 1, :] = value[0:1]
            edges[layer, half, 1, at : at + 1, :] = value[cols - 1 : cols]
        tails = jnp.concatenate([value[:, TILE:ch] for value in values], axis=1)
        act[layer, half, 2, row] = tails.astype(jnp.bfloat16)

    def spread(layer, kind):
        base = {LATE: 4, EARLY: 2, PAST: 0}[kind]
        for row in range(-1, rows + 1):
            if row < 0 or row >= rows:
                dy = 1 if row < 0 else -1
                source = row_in.at[layer, kind, (dy + 1) // 2]
                edge_row = rows - 1 if row < 0 else 0
            else:
                dy = 0
                source = main_in.at[layer, :, row] if kind == PAST else act.at[layer, kind, :, row]
                edge_row = row
            tails = source[2].astype(jnp.float32)
            for f in range(2):
                at = f * rows + edge_row
                slot = f * (rows + 2) + row + 1
                line[slot, 8 : 8 + cols, 0:TILE] = source[f].astype(jnp.float32)
                line[slot, 8 : 8 + cols, TILE:lanes] = pltpu.roll(tails, TILE // 2, 1) if f else tails
                line[slot, 7:8, 0:ch] = edge_in[layer, kind, dy + 1, 1, at : at + 1, :]
                line[slot, 8 + cols : 9 + cols, 0:ch] = edge_in[layer, kind, dy + 1, 0, at : at + 1, :]
                for r in range(3):
                    cols3[layer, base + f, row + 1, 0:cols, r * lanes : (r + 1) * lanes] = line[
                        slot, 7 + r : 7 + r + cols, :
                    ].astype(jnp.bfloat16)

    def convolve(layer, frame, own):
        total_at = acc.at[1 if frame else 0]

        def product(p):
            total = None
            for q in range(3):
                piece = cols3[layer, pl.ds(frame + p, 2), q : q + rows].reshape(-1, 3 * lanes)
                kernel = weights[layer, pl.ds(9 * p + 3 * q, 3)].reshape(3 * lanes, ch)
                part = jnp.dot(piece, kernel, preferred_element_type=jnp.float32)
                total = part if total is None else total + part
            return total

        def tap(p, _):
            total_at[...] += product(p)
            return 0

        if own:
            total_at[...] = product(2)
        else:
            lax.fori_loop(0, 2, tap, 0)

    def cells(half, f, row):
        at = (f * rows + row) * colsp
        return acc[1 - half, at : at + cols, :]

    def middle(half):
        for row in range(rows):
            values = []
            for f in range(2):
                value = (cells(half, f, row) + bias1[...]).astype(jnp.bfloat16).astype(jnp.float32)
                values.append(activate(value, gain2[...]))
            keep(1, half, row, values)

    def finish(half):
        frame = 0 if half == EARLY else 2
        for f in range(2):
            for row in range(rows):
                value = (cells(half, f, row) + bias2[...]).T + feat[frame + f, row].astype(jnp.float32)
                out[frame + f, row] = value.astype(jnp.bfloat16)

    def first(half):
        frame = 0 if half == EARLY else 2
        for row in range(rows):
            keep(0, half, row, [
                activate(feat[frame + f, row].astype(jnp.float32).T, gain1[...]) for f in range(2)
            ])

    edges[...] = jnp.zeros_like(edges)
    first(LATE)
    pl.semaphore_wait(barrier, expected)
    send_late(0)
    first(EARLY)
    send_early(0)
    weights[:, :, ch:, :] = jnp.zeros((2, weights.shape[1], lanes - ch, ch), jnp.bfloat16)
    line[...] = jnp.zeros_like(line)
    receive(0, LATE, moves_of(LATE))
    spread(0, LATE)
    w_copies[0].wait()
    convolve(0, 2, True)
    receive(0, EARLY, moves_of(EARLY))
    spread(0, EARLY)
    convolve(0, 2, False)
    middle(LATE)
    send_late(1)
    convolve(0, 0, True)
    w_copies[1].wait()
    receive(1, LATE, moves_of(LATE))
    spread(1, LATE)
    convolve(1, 2, True)
    receive_past(0)
    spread(0, PAST)
    convolve(0, 0, False)
    middle(EARLY)
    send_early(1)
    receive(1, EARLY, moves_of(EARLY))
    spread(1, EARLY)
    convolve(1, 2, False)
    finish(LATE)
    convolve(1, 0, True)
    receive_past(1)
    spread(1, PAST)
    convolve(1, 0, False)
    finish(EARLY)
    for layer in range(2):
        for kind in (LATE, EARLY, PAST):
            for dy, dx in moves_of(kind):
                ok, copy = copy_of(layer, kind, dy, dx)
                pl.when(ok)(copy.wait_send)


def local(features, gain_first, kernel_first, bias_first, gain_second, kernel_second, bias_second):
    frames, rows, cols, ch = features.shape
    colsp = -(-cols // 16) * 16
    lanes = -(-ch // 128) * 128
    vmem = pl.BlockSpec(memory_space=pltpu.VMEM)
    hbm = pl.BlockSpec(memory_space=pl.ANY)
    edge_rows = -(-2 * rows // 8) * 8
    bf16, f32 = jnp.bfloat16, jnp.float32
    result = pl.pallas_call(
        block_kernel,
        out_shape=jax.ShapeDtypeStruct((frames, rows, ch, cols), bf16),
        in_specs=[vmem] * 5 + [hbm] * 2,
        out_specs=vmem,
        scratch_shapes=[
            pltpu.VMEM((2, 27, lanes, ch), bf16),
            pltpu.VMEM((2, 2, 3, rows, cols, TILE), bf16),
            pltpu.VMEM((2, 2, 2, edge_rows, ch), f32),
            pltpu.VMEM((2, 3, rows, cols, TILE), bf16),
            pltpu.VMEM((2, 3, 2, 3, cols, TILE), bf16),
            pltpu.VMEM((2, 3, 3, 2, edge_rows, ch), f32),
            pltpu.VMEM((2 * (rows + 2), cols + 16, lanes), f32),
            pltpu.VMEM((2, frames + 2, rows + 2, colsp, 3 * lanes), bf16),
            pltpu.VMEM((2, 2 * rows * colsp, ch), f32),
            pltpu.SemaphoreType.DMA((2,)),
            pltpu.SemaphoreType.DMA((2, 27)),
            pltpu.SemaphoreType.DMA((2, 27)),
        ],
        compiler_params=pltpu.CompilerParams(
            collective_id=0, has_side_effects=True, vmem_limit_bytes=56 * 1024 * 1024
        ),
        name="residual_block",
    )(
        jnp.swapaxes(features, 2, 3),
        gain_first.reshape(1, ch),
        bias_first.reshape(1, ch),
        gain_second.reshape(1, ch),
        bias_second.reshape(1, ch),
        kernel_first.reshape(27, ch, ch),
        kernel_second.reshape(27, ch, ch),
    )
    return jnp.swapaxes(result, 2, 3)


def solution(mesh):
    placed = (P("ta", "gy", "gx", None), P(), P(), P(), P(), P(), P())
    return jax.shard_map(
        local, mesh=mesh, in_specs=placed, out_specs=P("ta", "gy", "gx", None), check_vma=False
    )
```

```python
import functools

import jax
import jax.numpy as jnp
from jax import lax
from jax.experimental import pallas as pl
from jax.experimental.pallas import tpu as pltpu
from jax.sharding import PartitionSpec as P

epsilon = 1e-06
LATE, EARLY, PAST = 0, 1, 2
TILE = 128
MOVES = [(dy, dx) for dy in (-1, 0, 1) for dx in (-1, 0, 1)]


def moves_of(kind):
    return [m for m in MOVES if (kind == PAST) == (m == (0, 0))]


def activate(field, gain):
    meansq = jnp.mean(field * field, axis=-1, keepdims=True)
    u = field * lax.rsqrt(meansq + epsilon) * gain
    return u / (1.0 + jnp.exp(-u))


def block_kernel(
    feat, gain1, bias1, gain2, bias2, k1, k2, out,
    weights, act, edges, main_out, main_in, row_in, edge_in, line, cols3, acc,
    w_sem, send_sem, recv_sem,
):
    rows, ch, cols = feat.shape[1:]
    colsp = acc.shape[1] // (2 * rows)
    lanes = line.shape[-1]
    ta, gy, gx = (lax.axis_index(a) for a in ("ta", "gy", "gx"))
    n_ta, n_gy, n_gx = (lax.axis_size(a) for a in ("ta", "gy", "gx"))

    def inside(kind, dy, dx, sign):
        t = ta + sign * (1 if kind == PAST else 0)
        y, x = gy + sign * dy, gx + sign * dx
        ok = (t >= 0) & (t < n_ta) & (y >= 0) & (y < n_gy) & (x >= 0) & (x < n_gx)
        return ok, {"ta": t, "gy": y, "gx": x}

    w_copies = [
        pltpu.make_async_copy(k, weights.at[layer, :, pl.ds(0, ch)], w_sem.at[layer])
        for layer, k in enumerate((k1, k2))
    ]
    w_copies[0].start()
    w_copies[1].start()

    barrier = pltpu.get_barrier_semaphore()
    expected = jnp.int32(0)
    for kind in (LATE, PAST):
        for dy, dx in moves_of(kind):
            ok, source = inside(kind, dy, dx, -1)

            @pl.when(ok)
            def _():
                pl.semaphore_signal(
                    barrier, inc=1, device_id=source, device_id_type=pl.DeviceIdType.MESH
                )

            expected = expected + inside(kind, dy, dx, 1)[0].astype(jnp.int32)

    def landing(layer, kind, dy, dx):
        if dx:
            return edge_in.at[layer, kind, dy + 1, (dx + 1) // 2]
        if dy:
            return row_in.at[layer, kind, (dy + 1) // 2]
        return main_in.at[layer]

    def copy_of(layer, kind, dy, dx):
        half = EARLY if kind == EARLY else LATE
        if dx:
            src = edges.at[layer, half, (dx + 1) // 2]
        elif dy:
            src = act.at[layer, half, :, rows - 1 if dy > 0 else 0]
        else:
            src = main_out.at[layer]
        number = kind * 9 + (dy + 1) * 3 + dx + 1
        ok, target = inside(kind, dy, dx, 1)
        return ok, pltpu.make_async_remote_copy(
            src_ref=src,
            dst_ref=landing(layer, kind, dy, dx),
            send_sem=send_sem.at[layer, number],
            recv_sem=recv_sem.at[layer, number],
            device_id=target,
            device_id_type=pl.DeviceIdType.MESH,
        )

    def send(layer, moves):
        for kind, dy, dx in moves:
            ok, copy = copy_of(layer, kind, dy, dx)
            pl.when(ok)(copy.start)

    def send_rim(layer, half):
        send(layer, [(half, *m) for m in sorted(moves_of(half), key=lambda m: (m[1] != 0, m))])

    def receive(layer, kind, moves):
        for dy, dx in moves:
            ok, _ = inside(kind, dy, dx, -1)
            copy = copy_of(layer, kind, dy, dx)[1]
            place = landing(layer, kind, dy, dx)
            pl.when(ok)(copy.wait_recv)

            @pl.when(jnp.logical_not(ok))
            def _():
                place[...] = jnp.zeros_like(place)

    def keep(layer, half, row, values):
        for f, value in enumerate(values):
            packed = value.astype(jnp.bfloat16)
            act[layer, half, f, row] = packed[:, 0:TILE]
            value = packed.astype(jnp.float32)
            at = f * rows + row
            edges[layer, half, 0, at : at + 1, :] = value[0:1]
            edges[layer, half, 1, at : at + 1, :] = value[cols - 1 : cols]
        tails = jnp.concatenate([value[:, TILE:ch] for value in values], axis=1)
        act[layer, half, 2, row] = tails.astype(jnp.bfloat16)

    def spread(layer, kind):
        base = 4 if kind == LATE else 2
        for row in range(-1, rows + 1):
            if row < 0 or row >= rows:
                dy = 1 if row < 0 else -1
                source = row_in.at[layer, kind, (dy + 1) // 2]
                edge_row = rows - 1 if row < 0 else 0
            else:
                dy = 0
                source = act.at[layer, kind, :, row]
                edge_row = row
            tails = source[2].astype(jnp.float32)
            for f in range(2):
                at = f * rows + edge_row
                slot = f * (rows + 2) + row + 1
                line[slot, 8 : 8 + cols, 0:TILE] = source[f].astype(jnp.float32)
                line[slot, 8 : 8 + cols, TILE:lanes] = pltpu.roll(tails, TILE // 2, 1) if f else tails
                line[slot, 7:8, 0:ch] = edge_in[layer, kind, dy + 1, 1, at : at + 1, :]
                line[slot, 8 + cols : 9 + cols, 0:ch] = edge_in[layer, kind, dy + 1, 0, at : at + 1, :]
                for r in range(3):
                    cols3[layer, base + f, row + 1, 0:cols, r * lanes : (r + 1) * lanes] = line[
                        slot, 7 + r : 7 + r + cols, :
                    ].astype(jnp.bfloat16)

    def product(layer, frame, count, p):
        total = None
        for q in range(3):
            piece = cols3[layer, pl.ds(frame, count), q : q + rows].reshape(-1, 3 * lanes)
            kernel = weights[layer, pl.ds(9 * p + 3 * q, 3)].reshape(3 * lanes, ch)
            part = jnp.dot(piece, kernel, preferred_element_type=jnp.float32)
            total = part if total is None else total + part
        return total

    area = rows * colsp

    def convolve_late(layer, own):
        def tap(p, _):
            acc[1] += product(layer, 2 + p, 2, p)
            return 0

        if own:
            acc[1] = product(layer, 4, 2, 2)
        else:
            lax.fori_loop(0, 2, tap, 0)

    def convolve_early(layer):
        acc[0] = product(layer, 2, 2, 2)
        acc[0, area:] += product(layer, 2, 1, 1)

    def hand_on(layer):
        acc[2] = product(layer, 4, 2, 0)
        acc[2, :area] += product(layer, 5, 1, 1)
        for row in range(rows):
            values = [acc[2, pl.ds((f * rows + row) * colsp, cols)] for f in range(2)]
            for f, value in enumerate(values):
                main_out[layer, f, row] = value[:, 0:TILE].astype(jnp.bfloat16)
            tails = jnp.concatenate([value[:, TILE:ch] for value in values], axis=1)
            main_out[layer, 2, row] = tails.astype(jnp.bfloat16)
        send(layer, [(PAST, 0, 0)])

    def add_past(layer):
        receive(layer, PAST, [(0, 0)])
        for row in range(rows):
            tails = main_in[layer, 2, row].astype(jnp.float32)
            for f in range(2):
                at = (f * rows + row) * colsp
                acc[0, at : at + cols, 0:TILE] += main_in[layer, f, row].astype(jnp.float32)
                tail = pltpu.roll(tails, TILE // 2, 1) if f else tails
                acc[0, at : at + cols, TILE:ch] += tail[:, 0 : ch - TILE]

    def cells(half, f, row):
        at = (f * rows + row) * colsp
        return acc[1 - half, at : at + cols, :]

    def middle(half):
        for row in range(rows):
            values = []
            for f in range(2):
                value = (cells(half, f, row) + bias1[...]).astype(jnp.bfloat16).astype(jnp.float32)
                values.append(activate(value, gain2[...]))
            keep(1, half, row, values)

    def finish(half):
        frame = 0 if half == EARLY else 2
        for f in range(2):
            for row in range(rows):
                value = (cells(half, f, row) + bias2[...]).T + feat[frame + f, row].astype(jnp.float32)
                out[frame + f, row] = value.astype(jnp.bfloat16)

    def first(half):
        frame = 0 if half == EARLY else 2
        for row in range(rows):
            keep(0, half, row, [
                activate(feat[frame + f, row].astype(jnp.float32).T, gain1[...]) for f in range(2)
            ])

    edges[...] = jnp.zeros_like(edges)
    first(LATE)
    pl.semaphore_wait(barrier, expected)
    send_rim(0, LATE)
    first(EARLY)
    send_rim(0, EARLY)
    weights[:, :, ch:, :] = jnp.zeros((2, weights.shape[1], lanes - ch, ch), jnp.bfloat16)
    line[...] = jnp.zeros_like(line)
    receive(0, LATE, moves_of(LATE))
    spread(0, LATE)
    w_copies[0].wait()
    hand_on(0)
    receive(0, EARLY, moves_of(EARLY))
    spread(0, EARLY)
    convolve_late(0, True)
    convolve_late(0, False)
    middle(LATE)
    send_rim(1, LATE)
    convolve_early(0)
    w_copies[1].wait()
    receive(1, LATE, moves_of(LATE))
    spread(1, LATE)
    hand_on(1)
    add_past(0)
    middle(EARLY)
    send_rim(1, EARLY)
    convolve_late(1, True)
    receive(1, EARLY, moves_of(EARLY))
    spread(1, EARLY)
    convolve_late(1, False)
    finish(LATE)
    convolve_early(1)
    add_past(1)
    finish(EARLY)
    for layer in range(2):
        for kind in (LATE, EARLY, PAST):
            for dy, dx in moves_of(kind):
                ok, copy = copy_of(layer, kind, dy, dx)
                pl.when(ok)(copy.wait_send)


def local(features, gain_first, kernel_first, bias_first, gain_second, kernel_second, bias_second):
    frames, rows, cols, ch = features.shape
    colsp = -(-cols // 16) * 16
    lanes = -(-ch // 128) * 128
    vmem = pl.BlockSpec(memory_space=pltpu.VMEM)
    hbm = pl.BlockSpec(memory_space=pl.ANY)
    edge_rows = -(-2 * rows // 8) * 8
    bf16, f32 = jnp.bfloat16, jnp.float32
    result = pl.pallas_call(
        block_kernel,
        out_shape=jax.ShapeDtypeStruct((frames, rows, ch, cols), bf16),
        in_specs=[vmem] * 5 + [hbm] * 2,
        out_specs=vmem,
        scratch_shapes=[
            pltpu.VMEM((2, 27, lanes, ch), bf16),
            pltpu.VMEM((2, 2, 3, rows, cols, TILE), bf16),
            pltpu.VMEM((2, 2, 2, edge_rows, ch), f32),
            pltpu.VMEM((2, 3, rows, cols, TILE), bf16),
            pltpu.VMEM((2, 3, rows, cols, TILE), bf16),
            pltpu.VMEM((2, 2, 2, 3, cols, TILE), bf16),
            pltpu.VMEM((2, 2, 3, 2, edge_rows, ch), f32),
            pltpu.VMEM((2 * (rows + 2), cols + 16, lanes), f32),
            pltpu.VMEM((2, frames + 2, rows + 2, colsp, 3 * lanes), bf16),
            pltpu.VMEM((3, 2 * rows * colsp, ch), f32),
            pltpu.SemaphoreType.DMA((2,)),
            pltpu.SemaphoreType.DMA((2, 27)),
            pltpu.SemaphoreType.DMA((2, 27)),
        ],
        compiler_params=pltpu.CompilerParams(
            collective_id=0, has_side_effects=True, vmem_limit_bytes=56 * 1024 * 1024
        ),
        name="residual_block",
    )(
        jnp.swapaxes(features, 2, 3),
        gain_first.reshape(1, ch),
        bias_first.reshape(1, ch),
        gain_second.reshape(1, ch),
        bias_second.reshape(1, ch),
        kernel_first.reshape(27, ch, ch),
        kernel_second.reshape(27, ch, ch),
    )
    return jnp.swapaxes(result, 2, 3)


def solution(mesh):
    placed = (P("ta", "gy", "gx", None), P(), P(), P(), P(), P(), P())
    return jax.shard_map(
        local, mesh=mesh, in_specs=placed, out_specs=P("ta", "gy", "gx", None), check_vma=False
    )
```

```python
import functools

import jax
import jax.numpy as jnp
from jax import lax
from jax.experimental import pallas as pl
from jax.experimental.pallas import tpu as pltpu
from jax.sharding import PartitionSpec as P

epsilon = 1e-06
LATE, EARLY, PAST = 0, 1, 2
TILE = 128
MOVES = [(dy, dx) for dy in (-1, 0, 1) for dx in (-1, 0, 1)]


def moves_of(kind):
    return [m for m in MOVES if (kind == PAST) == (m == (0, 0))]


def activate(field, gain):
    meansq = jnp.mean(field * field, axis=-1, keepdims=True)
    u = field * lax.rsqrt(meansq + epsilon) * gain
    return u / (1.0 + jnp.exp(-u))


def block_kernel(
    feat, gain1, bias1, gain2, bias2, k1, k2, out,
    weights, act, edges, main_out, main_in, row_in, edge_in, line, cols3, acc,
    w_sem, send_sem, recv_sem,
):
    rows, ch, cols = feat.shape[1:]
    colsp = acc.shape[1] // (2 * rows)
    lanes = line.shape[-1]
    ta, gy, gx = (lax.axis_index(a) for a in ("ta", "gy", "gx"))
    n_ta, n_gy, n_gx = (lax.axis_size(a) for a in ("ta", "gy", "gx"))

    def inside(kind, dy, dx, sign):
        t = ta + sign * (1 if kind == PAST else 0)
        y, x = gy + sign * dy, gx + sign * dx
        ok = (t >= 0) & (t < n_ta) & (y >= 0) & (y < n_gy) & (x >= 0) & (x < n_gx)
        return ok, {"ta": t, "gy": y, "gx": x}

    w_copies = [
        pltpu.make_async_copy(k, weights.at[layer, :, pl.ds(0, ch)], w_sem.at[layer])
        for layer, k in enumerate((k1, k2))
    ]
    w_copies[0].start()
    w_copies[1].start()

    barrier = pltpu.get_barrier_semaphore()
    expected = jnp.int32(0)
    for kind in (LATE, PAST):
        for dy, dx in moves_of(kind):
            ok, source = inside(kind, dy, dx, -1)

            @pl.when(ok)
            def _():
                pl.semaphore_signal(
                    barrier, inc=1, device_id=source, device_id_type=pl.DeviceIdType.MESH
                )

            expected = expected + inside(kind, dy, dx, 1)[0].astype(jnp.int32)

    def landing(layer, kind, dy, dx):
        if dx:
            return edge_in.at[layer, kind, dy + 1, (dx + 1) // 2]
        if dy:
            return row_in.at[layer, kind, (dy + 1) // 2]
        return main_in.at[layer]

    def copy_of(layer, kind, dy, dx):
        half = EARLY if kind == EARLY else LATE
        if dx:
            src = edges.at[layer, half, (dx + 1) // 2]
        elif dy:
            src = act.at[layer, half, :, rows - 1 if dy > 0 else 0]
        else:
            src = main_out.at[layer]
        number = kind * 9 + (dy + 1) * 3 + dx + 1
        ok, target = inside(kind, dy, dx, 1)
        return ok, pltpu.make_async_remote_copy(
            src_ref=src,
            dst_ref=landing(layer, kind, dy, dx),
            send_sem=send_sem.at[layer, number],
            recv_sem=recv_sem.at[layer, number],
            device_id=target,
            device_id_type=pl.DeviceIdType.MESH,
        )

    def send(layer, moves):
        for kind, dy, dx in moves:
            ok, copy = copy_of(layer, kind, dy, dx)
            pl.when(ok)(copy.start)

    def send_rim(layer, half):
        send(layer, [(half, *m) for m in sorted(moves_of(half), key=lambda m: (m[1] != 0, m))])

    def receive(layer, kind, moves):
        for dy, dx in moves:
            ok, _ = inside(kind, dy, dx, -1)
            copy = copy_of(layer, kind, dy, dx)[1]
            place = landing(layer, kind, dy, dx)
            pl.when(ok)(copy.wait_recv)

            @pl.when(jnp.logical_not(ok))
            def _():
                place[...] = jnp.zeros_like(place)

    def keep(layer, half, row, values):
        for f, value in enumerate(values):
            packed = value.astype(jnp.bfloat16)
            act[layer, half, f, row] = packed[:, 0:TILE]
            value = packed.astype(jnp.float32)
            at = f * rows + row
            edges[layer, half, 0, at : at + 1, :] = value[0:1]
            edges[layer, half, 1, at : at + 1, :] = value[cols - 1 : cols]
        tails = jnp.concatenate([value[:, TILE:ch] for value in values], axis=1)
        act[layer, half, 2, row] = tails.astype(jnp.bfloat16)

    def spread(layer, kind):
        base = 4 if kind == LATE else 2
        for row in range(-1, rows + 1):
            if row < 0 or row >= rows:
                dy = 1 if row < 0 else -1
                source = row_in.at[layer, kind, (dy + 1) // 2]
                edge_row = rows - 1 if row < 0 else 0
            else:
                dy = 0
                source = act.at[layer, kind, :, row]
                edge_row = row
            tails = source[2].astype(jnp.float32)
            for f in range(2):
                at = f * rows + edge_row
                slot = f * (rows + 2) + row + 1
                line[slot, 8 : 8 + cols, 0:TILE] = source[f].astype(jnp.float32)
                line[slot, 8 : 8 + cols, TILE:lanes] = pltpu.roll(tails, TILE // 2, 1) if f else tails
                line[slot, 7:8, 0:ch] = edge_in[layer, kind, dy + 1, 1, at : at + 1, :]
                line[slot, 8 + cols : 9 + cols, 0:ch] = edge_in[layer, kind, dy + 1, 0, at : at + 1, :]
                for r in range(3):
                    cols3[layer, base + f, row + 1, 0:cols, r * lanes : (r + 1) * lanes] = line[
                        slot, 7 + r : 7 + r + cols, :
                    ].astype(jnp.bfloat16)

    def product(layer, frame, count, p):
        total = None
        for q in range(3):
            piece = cols3[layer, pl.ds(frame, count), q : q + rows].reshape(-1, 3 * lanes)
            kernel = weights[layer, pl.ds(9 * p + 3 * q, 3)].reshape(3 * lanes, ch)
            part = jnp.dot(piece, kernel, preferred_element_type=jnp.float32)
            total = part if total is None else total + part
        return total

    area = rows * colsp

    def convolve_late(layer, own):
        if own:
            acc[1] = product(layer, 4, 2, 2)
        else:
            acc[1] += product(layer, 2, 2, 0) + product(layer, 3, 2, 1)

    def convolve_early(layer):
        acc[0] = product(layer, 2, 2, 2)
        acc[0, area:] += product(layer, 2, 1, 1)

    def hand_on(layer):
        acc[2] = product(layer, 4, 2, 0)
        acc[2, :area] += product(layer, 5, 1, 1)
        for row in range(rows):
            values = [acc[2, pl.ds((f * rows + row) * colsp, cols)] for f in range(2)]
            for f, value in enumerate(values):
                main_out[layer, f, row] = value[:, 0:TILE].astype(jnp.bfloat16)
            tails = jnp.concatenate([value[:, TILE:ch] for value in values], axis=1)
            main_out[layer, 2, row] = tails.astype(jnp.bfloat16)
        send(layer, [(PAST, 0, 0)])

    def add_past(layer):
        receive(layer, PAST, [(0, 0)])
        for row in range(rows):
            tails = main_in[layer, 2, row].astype(jnp.float32)
            for f in range(2):
                at = (f * rows + row) * colsp
                acc[0, at : at + cols, 0:TILE] += main_in[layer, f, row].astype(jnp.float32)
                tail = pltpu.roll(tails, TILE // 2, 1) if f else tails
                acc[0, at : at + cols, TILE:ch] += tail[:, 0 : ch - TILE]

    def cells(half, f, row):
        at = (f * rows + row) * colsp
        return acc[1 - half, at : at + cols, :]

    def middle(half):
        for row in range(rows):
            values = []
            for f in range(2):
                value = (cells(half, f, row) + bias1[...]).astype(jnp.bfloat16).astype(jnp.float32)
                values.append(activate(value, gain2[...]))
            keep(1, half, row, values)

    def finish(half):
        frame = 0 if half == EARLY else 2
        for f in range(2):
            for row in range(rows):
                value = (cells(half, f, row) + bias2[...]).T + feat[frame + f, row].astype(jnp.float32)
                out[frame + f, row] = value.astype(jnp.bfloat16)

    def first(half):
        frame = 0 if half == EARLY else 2
        for row in range(rows):
            keep(0, half, row, [
                activate(feat[frame + f, row].astype(jnp.float32).T, gain1[...]) for f in range(2)
            ])

    edges[...] = jnp.zeros_like(edges)
    first(LATE)
    pl.semaphore_wait(barrier, expected)
    send_rim(0, LATE)
    first(EARLY)
    send_rim(0, EARLY)
    weights[:, :, ch:, :] = jnp.zeros((2, weights.shape[1], lanes - ch, ch), jnp.bfloat16)
    line[...] = jnp.zeros_like(line)
    receive(0, LATE, moves_of(LATE))
    spread(0, LATE)
    w_copies[0].wait()
    hand_on(0)
    receive(0, EARLY, moves_of(EARLY))
    spread(0, EARLY)
    convolve_late(0, True)
    convolve_late(0, False)
    middle(LATE)
    send_rim(1, LATE)
    convolve_early(0)
    w_copies[1].wait()
    receive(1, LATE, moves_of(LATE))
    spread(1, LATE)
    hand_on(1)
    add_past(0)
    middle(EARLY)
    send_rim(1, EARLY)
    convolve_late(1, True)
    receive(1, EARLY, moves_of(EARLY))
    spread(1, EARLY)
    convolve_late(1, False)
    finish(LATE)
    convolve_early(1)
    add_past(1)
    finish(EARLY)
    for layer in range(2):
        for kind in (LATE, EARLY, PAST):
            for dy, dx in moves_of(kind):
                ok, copy = copy_of(layer, kind, dy, dx)
                pl.when(ok)(copy.wait_send)


def local(features, gain_first, kernel_first, bias_first, gain_second, kernel_second, bias_second):
    frames, rows, cols, ch = features.shape
    colsp = -(-cols // 16) * 16
    lanes = -(-ch // 128) * 128
    vmem = pl.BlockSpec(memory_space=pltpu.VMEM)
    hbm = pl.BlockSpec(memory_space=pl.ANY)
    edge_rows = -(-2 * rows // 8) * 8
    bf16, f32 = jnp.bfloat16, jnp.float32
    result = pl.pallas_call(
        block_kernel,
        out_shape=jax.ShapeDtypeStruct((frames, rows, ch, cols), bf16),
        in_specs=[vmem] * 5 + [hbm] * 2,
        out_specs=vmem,
        scratch_shapes=[
            pltpu.VMEM((2, 27, lanes, ch), bf16),
            pltpu.VMEM((2, 2, 3, rows, cols, TILE), bf16),
            pltpu.VMEM((2, 2, 2, edge_rows, ch), f32),
            pltpu.VMEM((2, 3, rows, cols, TILE), bf16),
            pltpu.VMEM((2, 3, rows, cols, TILE), bf16),
            pltpu.VMEM((2, 2, 2, 3, cols, TILE), bf16),
            pltpu.VMEM((2, 2, 3, 2, edge_rows, ch), f32),
            pltpu.VMEM((2 * (rows + 2), cols + 16, lanes), f32),
            pltpu.VMEM((2, frames + 2, rows + 2, colsp, 3 * lanes), bf16),
            pltpu.VMEM((3, 2 * rows * colsp, ch), f32),
            pltpu.SemaphoreType.DMA((2,)),
            pltpu.SemaphoreType.DMA((2, 27)),
            pltpu.SemaphoreType.DMA((2, 27)),
        ],
        compiler_params=pltpu.CompilerParams(
            collective_id=0, has_side_effects=True, vmem_limit_bytes=56 * 1024 * 1024
        ),
        name="residual_block",
    )(
        jnp.swapaxes(features, 2, 3),
        gain_first.reshape(1, ch),
        bias_first.reshape(1, ch),
        gain_second.reshape(1, ch),
        bias_second.reshape(1, ch),
        kernel_first.reshape(27, ch, ch),
        kernel_second.reshape(27, ch, ch),
    )
    return jnp.swapaxes(result, 2, 3)


def solution(mesh):
    placed = (P("ta", "gy", "gx", None), P(), P(), P(), P(), P(), P())
    return jax.shard_map(
        local, mesh=mesh, in_specs=placed, out_specs=P("ta", "gy", "gx", None), check_vma=False
    )
```
